32 devices in a mesh: grp: 4 (over z), col: 8 (over y, x, core).
Axes of the slice: x: 2, y: 2, z: 4, core: 2. Of those that a mesh axis runs over, the one named last changes fastest.
Arguments:
- x_blocks: bfloat16 [16, 8, 6, 256, 256], P('grp', 'col'), may hold values from -6 to 6
- columns: int32 [16, 8, 6], replicated, may hold values from -1 to 127, as said below
- filter_ids: int32 [16, 8, 6], replicated, may hold values from 0 to 127, as said below
Outputs:
- sign_step: bfloat16 [16, 8, 6, 256, 256], P('grp', 'col')
The draws below stay inside these ranges and needn't reach their ends.
Inputs may be any that keep to these rules, and one draw needn't show every extreme that they name: `columns`: in each block row of the grid, slot 0 holds the row's own id; the other used slots hold distinct ids of block rows at most one step away along each grid dimension, with periodic wrap; used slots come first, then -1; at least 3 slots are used. `filter_ids`: in each block row, slot 0 holds the row's own id and the others distinct ids of block rows at most one step away along each grid dimension, with periodic wrap.
All inputs are finite; a program needn't handle non-finite values.
Results may differ from the reference program's by a relative error of at most 0.0019.
Values may be sent and summed in bfloat16 or wider, within the bound.
No kernel may reach another device: no remote copies, remote signals or barrier semaphores. Data moves between devices by JAX's collectives and lax.ppermute only.
A program may use at most 128 MiB of HBM per device.

```python
import jax
import jax.numpy as jnp
from jax import lax

B = 256
KB = 6
KF = 6
NA = 16
NBC = 8


def neighbour_ids(key, slots):
    total_rows = NA * NBC
    row_keys = jax.random.split(key, total_rows)
    shuffled = jax.vmap(lambda one_key: jax.random.permutation(one_key, 8))(row_keys)
    others = shuffled + (shuffled >= 4).astype(shuffled.dtype)
    offset_code = jnp.concatenate([jnp.full((total_rows, 1), 4, jnp.int32), others.astype(jnp.int32)], axis=1)[:, :slots]
    step_a = offset_code // 3 - 1
    step_c = offset_code % 3 - 1
    row_index = jnp.arange(total_rows, dtype=jnp.int32)
    home_a = row_index // NBC
    home_c = row_index % NBC
    block_ids = (home_a[:, None] + step_a) % NA * NBC + (home_c[:, None] + step_c) % NBC
    return block_ids.astype(jnp.int32)


def draw_columns(key, part):
    total_rows = NA * NBC
    block_ids = neighbour_ids(jax.random.fold_in(key, 11), KB)
    counts = jax.random.randint(jax.random.fold_in(key, 12), (total_rows, 1), 3, KB + 1)
    slot_index = jnp.arange(KB, dtype=jnp.int32)[None, :]
    block_ids = jnp.where(slot_index < counts, block_ids, -1)
    return block_ids.reshape(NA, NBC, KB).astype(jnp.int32)


def draw_filter_ids(key, part):
    block_ids = neighbour_ids(jax.random.fold_in(key, 21), KF)
    return block_ids.reshape(NA, NBC, KF).astype(jnp.int32)


def level_of(stream_key, shape, pieces, low, top_value):
    gain = 1.0
    for axis_at, blocks in pieces:
        draws = jax.random.uniform(jax.random.fold_in(jax.random.fold_in(stream_key, 6), axis_at), (blocks,), jnp.float32, low / len(pieces), top_value / len(pieces))
        gain = gain * jnp.repeat(jnp.exp(draws), shape[axis_at] // blocks).reshape((-1,) + (1,) * (len(shape) - 1 - axis_at))
    return gain


def bell_draw(key, shape, scale, most, cuts=(), kind=jnp.bfloat16):
    loudness = level_of(key, shape, cuts, -0.22, 0.18) if cuts else 1.0
    values = jax.random.normal(key, shape, jnp.float32) * scale * loudness
    return jnp.minimum(jnp.maximum(values, -most), most).astype(kind)


def setup_inputs(seed: int = 0) -> dict:
    key_of = jax.random.split(jax.random.key(seed), 4)
    return {
        "x_blocks": bell_draw(key_of[0], (NA, NBC, KB, B, B), 1.0, 6.0, ((0, 4), (1, 8))),
        "columns": draw_columns(jax.random.fold_in(key_of[3], 71), 0),
        "filter_ids": draw_filter_ids(jax.random.fold_in(key_of[3], 71), 0),
    }


def locate(stored, wanted):
    matches = stored[:, None, :] == wanted[None, :, None]
    present = jnp.any(matches, axis=2) & (wanted[None, :] >= 0)
    slot_of = jnp.argmax(matches.astype(jnp.int32), axis=2).astype(jnp.int32)
    return slot_of, present


def reference(x_blocks, columns, filter_ids):
    total_rows = NA * NBC
    blocks = x_blocks.reshape(total_rows, KB, B, B)
    col_table = columns.reshape(total_rows, KB)
    filt_table = filter_ids.reshape(total_rows, KF)

    def square_row(row_index):
        row_cols = col_table[row_index]
        in_use = row_cols >= 0
        source = jnp.where(in_use, row_cols, 0)
        slot_of, present = locate(col_table[source], filt_table[row_index])
        present = present & in_use[:, None]
        picked = blocks[source[:, None], slot_of].astype(jnp.float32) * present[:, :, None, None].astype(jnp.float32)
        own = blocks[row_index].astype(jnp.float32)
        return jnp.einsum("kab,kfbc->fac", own, picked).astype(jnp.bfloat16)

    square = lax.map(square_row, jnp.arange(total_rows, dtype=jnp.int32))

    def sign_row(row_index):
        row_cols = col_table[row_index]
        in_use = row_cols >= 0
        source = jnp.where(in_use, row_cols, 0)
        slot_of, present = locate(filt_table[source], row_cols)
        present = present & in_use[:, None]
        picked = square[source[:, None], slot_of].astype(jnp.float32) * present[:, :, None, None].astype(jnp.float32)
        own = blocks[row_index].astype(jnp.float32)
        cubed = jnp.einsum("kab,kjbc->jac", own, picked)
        result = (1.5 * own - cubed * (0.5 / (KB * B))) * in_use[:, None, None].astype(jnp.float32)
        return result.astype(jnp.bfloat16)

    updated = lax.map(sign_row, jnp.arange(total_rows, dtype=jnp.int32))
    return updated.reshape(NA, NBC, KB, B, B)
```

```python
import functools

import jax
import jax.numpy as jnp
from jax import lax
from jax.experimental import pallas as pl
from jax.experimental.pallas import tpu as pltpu
from jax.sharding import PartitionSpec as P

FIRST = (10, 12)
SECOND = ((4, 6, 8), (4, 6, 8))

ANY = pl.BlockSpec(memory_space=pl.ANY)
SMEM = pl.BlockSpec(memory_space=pltpu.SMEM)
VMEM = pl.BlockSpec(memory_space=pltpu.VMEM)

LINE = 16
TERMS = 8


class Layout:
    def __init__(self, rows, slots, cols, groups):
        self.rows, self.slots, self.cols, self.groups = rows, slots, cols, groups
        self.grid_a = rows * groups
        self.own = rows * slots
        self.top = self.own
        self.bottom = self.own + slots
        self.side = self.own + 2 * slots
        self.off = 2 * self.side
        self.edge = 4 if slots > 4 else slots
        self.most = self.own + 2 * self.edge

    def line(self, a, c):
        a = jnp.where(a < 0, a + self.grid_a, jnp.where(a >= self.grid_a, a - self.grid_a, a))
        return (a * self.cols + c) * LINE

    def around(self, c):
        even = (c & 1) == 0
        partner = jnp.where(even, c + 1, c - 1)
        other = jnp.where(even, c - 1, c + 1)
        other = jnp.where(other < 0, self.cols - 1, jnp.where(other >= self.cols, 0, other))
        return partner, other, jnp.where(even, 0, 2)


def edge_order(lay, tab, line, codes_at, off_code, first_da, put):
    fits = []
    for m in range(lay.slots):
        code = tab[line + codes_at + m]
        da = (code >= 5).astype(jnp.int32) + (code >= 10).astype(jnp.int32)
        dc = code - 5 * da
        ok = (code >= 0) & ((da == first_da) | (da == 1)) & ((dc == 1) | (dc == off_code))
        fits.append(ok.astype(jnp.int32))
    front, back = jnp.int32(0), sum(fits)
    for m in range(lay.slots):
        put(m, jnp.where(fits[m] == 1, front, back))
        front, back = front + fits[m], back + 1 - fits[m]


def used_masks(lay, tab, a0, consumer, source_code, target_at):
    masks = [jnp.int32(0)] * (lay.rows + 2)
    for i in range(lay.rows):
        line = lay.line(a0 + i, consumer)
        cols_mask = tab[line + 12]
        target = tab[line + target_at] << 6
        for da in range(3):
            code = da * 5 + source_code
            masks[i + da] = masks[i + da] | jnp.where(((cols_mask >> code) & 1) == 1, target >> code, 0)
    return masks


def used_list(lay, tab, a0, source, masks, codes_at, first, put):
    count = jnp.int32(0)
    for ii in [*range(1, lay.rows + 1), 0, lay.rows + 1]:
        if ii == 0:
            count = jnp.maximum(count, first)
        line = lay.line(a0 + ii - 1, source)
        for m in range(lay.slots):
            code = tab[line + codes_at + m]
            hit = ((masks[ii] >> jnp.maximum(code, 0)) & 1) * (code >= 0).astype(jnp.int32)
            put(hit, count, ii, m)
            count = count + hit


def send_plan(lay, here, tab, stage, first, ranks, sends, edges):
    g, c = here[0], here[1]
    _, other, off_code = lay.around(c)
    codes_at, target_at = (0, 13) if stage == 0 else (6, 12)
    a0 = g * lay.rows
    for which, (a, da) in enumerate(((a0 - 1, 2), (a0 + lay.rows, 0))):

        def put_rank(m, rank, at=which * 8):
            ranks[at + m] = rank

        edge_order(lay, tab, lay.line(a, c), codes_at, off_code, da, put_rank)
    for which, (row, da) in enumerate(((lay.rows - 1, 2), (0, 0))):

        def put_edge(m, rank, at=which * 8, row=row):
            edges[at + rank] = row * lay.slots + m

        edge_order(lay, tab, lay.line(a0 + row, c), codes_at, off_code, da, put_edge)
    for j in range(lay.most):
        sends[j] = 0

    def put(hit, count, ii, m):
        if ii == 0:
            index = lay.top + ranks[m]
        elif ii == lay.rows + 1:
            index = lay.bottom + ranks[8 + m]
        else:
            index = (ii - 1) * lay.slots + m

        @pl.when(hit == 1)
        def _():
            sends[count] = index

    masks = used_masks(lay, tab, a0, other, off_code_of_source(off_code), target_at)
    used_list(lay, tab, a0, c, masks, codes_at, first, put)


def off_code_of_source(off_code):
    return 2 - off_code


def term_plan(lay, here, tab, stage, first, place, slot_of, terms):
    g, c = here[0], here[1]
    partner, other, off_code = lay.around(c)
    codes_at, target_at, goal_at = (0, 13, 6) if stage == 0 else (6, 12, 0)
    a0 = g * lay.rows
    span = lay.rows + 2
    for side, column, own_off in ((0, c, off_code), (1, partner, 2 - off_code)):
        base = side * lay.side
        for ii in range(1, lay.rows + 1):
            for m in range(lay.slots):
                place[(side * span + ii) * 8 + m] = base + (ii - 1) * lay.slots + m
        for ii, da, start in ((0, 2, lay.top), (lay.rows + 1, 0, lay.bottom)):

            def put_rank(m, rank, at=(side * span + ii) * 8, start=base + start):
                place[at + m] = start + rank

            edge_order(lay, tab, lay.line(a0 + ii - 1, column), codes_at, own_off, da, put_rank)

    def put(hit, count, ii, m):
        place[(2 * span + ii) * 8 + m] = lay.off + count

    masks = used_masks(lay, tab, a0, c, off_code, target_at)
    used_list(lay, tab, a0, other, masks, codes_at, first, put)

    for i in range(lay.rows):
        line = lay.line(a0 + i, c)
        target = tab[line + target_at] << 6
        for f in range(lay.slots):
            code = tab[line + goal_at + f]
            at = (i * lay.slots + f) * TERMS
            terms[at] = 0
            terms[at + TERMS - 1] = (code >= 0).astype(jnp.int32)

            @pl.when(code >= 0)
            def _(code=code, f=f):
                slot_of[code] = f

        def one_slot(k, carry, i=i, line=line, target=target):
            code = tab[line + k]

            @pl.when(code >= 0)
            def _():
                da = (code >= 5).astype(jnp.int32) + (code >= 10).astype(jnp.int32)
                dc = code - 5 * da
                side = jnp.where(dc == 1, 0, jnp.where(dc == off_code, 2, 1))
                column = jnp.where(side == 0, c, jnp.where(side == 1, partner, other))
                source = lay.line(a0 + i + da - 1, column)
                place_at = (side * span + i + da) * 8
                wanted = target >> code
                for m in range(lay.slots):
                    there = tab[source + codes_at + m]
                    hit = ((wanted >> jnp.maximum(there, 0)) & 1) * (there >= 0).astype(jnp.int32)

                    @pl.when(hit == 1)
                    def _(there=there, m=m):
                        at = (i * lay.slots + slot_of[code + there - 6]) * TERMS
                        count = terms[at] + 1
                        terms[at] = count
                        terms[at + count] = (i * lay.slots + k) * 256 + place[place_at + m]

            return carry

        lax.fori_loop(0, lay.slots, one_slot, 0)


def needed_second(lay, vec, stage, first):
    shape = (8, vec.shape[1])
    cols_mask, filt_mask, i, c = (jnp.broadcast_to(vec[n : n + 1, :], shape) for n in range(4))
    stored, goal = (cols_mask, filt_mask) if stage == 0 else (filt_mask, cols_mask)
    total = shape[1]
    width = lay.cols

    def count(bits):
        return sum((bits >> (da * 5 + dc)) & 1 for da in range(3) for dc in range(3))

    def moved(value, by):
        return value if by % total == 0 else pltpu.roll(value, by % total, 1)

    most = jnp.zeros(shape, jnp.int32)
    for source_code in (0, 2):
        bits = []
        for da in range(3):
            code = da * 5 + source_code
            value = jnp.where(((cols_mask >> code) & 1) == 1, (goal << 6) >> code, 0)
            by = (da - 1) * width + source_code - 1
            wraps = c == (0 if source_code == 2 else width - 1)
            back = by - width if source_code == 2 else by + width
            bits.append(jnp.where(wraps, moved(value, back), moved(value, by)) & stored)
        beside = bits[1] | jnp.where(i < lay.rows - 1, bits[0], 0) | jnp.where(i > 0, bits[2], 0)
        beside = count(beside)
        top = count(jnp.where(i == lay.rows - 1, bits[0], 0))
        bottom = count(jnp.where(i == 0, bits[2], 0))
        sides = sum(moved(beside, -j * width) for j in range(lay.rows))
        corners = moved(top, width) + moved(bottom, -lay.rows * width)
        need = jnp.maximum(sides, first) + corners - first
        counts = (i == 0) & ((c & 1) == (0 if source_code == 2 else 1))
        most = jnp.maximum(most, jnp.where(counts, need, 0))
    return jnp.max(most)


def first_plan_body(lay, firsts, sizes, here, tab, vec, sends, edges, picks, ranks):
    send_plan(lay, here, tab, 0, firsts[0], ranks, sends, edges)
    for stage in range(2):
        need = needed_second(lay, vec[...], stage, firsts[stage])
        picks[stage] = sum((need > size).astype(jnp.int32) for size in sizes[stage][:-1])


def rest_plan_body(lay, firsts, here, tab, sends, edges, terms0, terms1, ranks, place, slot_of):
    send_plan(lay, here, tab, 1, firsts[1], ranks, sends, edges)
    term_plan(lay, here, tab, 0, firsts[0], place, slot_of, terms0)
    term_plan(lay, here, tab, 1, firsts[1], place, slot_of, terms1)


def ints(*shape):
    return jax.ShapeDtypeStruct(shape, jnp.int32)


def pack_body(parts, picks, sends, *refs):
    sources, rest = refs[: len(parts)], refs[len(parts) :]
    count = len(picks)
    outs, (held, sems_in, sems_out) = rest[:-3], rest[-3:]
    for j, (list_ref, at, _, _) in enumerate(picks):
        index = sends[list_ref][at]
        for source, (low, high) in zip(sources, parts):

            @pl.when((index >= low) & (index < high))
            def _(source=source, low=low, j=j, index=index):
                pltpu.make_async_copy(source.at[index - low], held.at[j], sems_in.at[j]).start()

    for j, (_, _, out, at_out) in enumerate(picks):
        pltpu.make_async_copy(sources[0].at[0], held.at[j], sems_in.at[j]).wait()
        pltpu.make_async_copy(held.at[j], outs[out].at[at_out], sems_out.at[j]).start()
    for j, (_, _, out, at_out) in enumerate(picks):
        pltpu.make_async_copy(held.at[j], outs[out].at[at_out], sems_out.at[j]).wait()


def pack(block, lists, sources, parts, sizes, picks):
    def body(*refs):
        pack_body(parts, picks, refs[: len(lists)], *refs[len(lists) :])

    return pl.pallas_call(
        body,
        out_shape=[jax.ShapeDtypeStruct((size, *block), jnp.bfloat16) for size in sizes],
        in_specs=[SMEM] * len(lists) + [ANY] * len(sources),
        out_specs=[ANY] * len(sizes),
        scratch_shapes=[
            pltpu.VMEM((len(picks), *block), jnp.bfloat16),
            pltpu.SemaphoreType.DMA((len(picks),)),
            pltpu.SemaphoreType.DMA((len(picks),)),
        ],
        cost_estimate=pl.CostEstimate(
            flops=1 << 20, bytes_accessed=4 * len(picks) * block[0] * block[1], transcendentals=0
        ),
    )(*lists, *sources)


def products(lay, terms, left, pool, finish):
    def one(o, carry):
        at = o * TERMS
        count = terms[at]
        for n in range(lay.slots + 1):

            @pl.when(count == n)
            def _(n=n):
                if n == 0:
                    finish(o, None)
                    return
                lefts, rights = [], []
                for e in range(n):
                    term = terms[at + 1 + e]
                    lefts.append(left[term >> 8])
                    rights.append(pool[term & 255])
                joined = lefts[0] if n == 1 else jnp.concatenate(lefts, axis=1)
                stacked = rights[0] if n == 1 else jnp.concatenate(rights, axis=0)
                finish(o, jnp.dot(joined, stacked, preferred_element_type=jnp.float32))

        return carry

    lax.fori_loop(0, lay.own, one, 0)


def load_pool(sources, starts, pool, sems):
    copies = [
        pltpu.make_async_copy(source, pool.at[pl.ds(start, source.shape[0])], sems.at[n])
        for n, (source, start) in enumerate(zip(sources, starts))
    ]
    for copy in copies:
        copy.start()
    return copies


def square_body(lay, starts, picks, terms, sends, edges, *refs):
    sources, rest = refs[: len(starts)], refs[len(starts) :]
    outs, (pool, square, sems, out_sems) = rest[:-4], rest[-4:]
    for copy in load_pool(sources, starts, pool, sems):
        copy.wait()

    def finish(o, total):
        if total is None:
            square[o] = jnp.zeros(square.shape[1:], square.dtype)
        else:
            square[o] = total.astype(square.dtype)

    products(lay, terms, pool, pool, finish)
    lists = (sends, edges)
    copies = [pltpu.make_async_copy(square, outs[0], out_sems.at[0])]
    for j, (list_at, at, out, at_out) in enumerate(picks):
        copies.append(
            pltpu.make_async_copy(
                square.at[lists[list_at][at]], outs[out + 1].at[at_out], out_sems.at[j + 1]
            )
        )
    for copy in copies[1:]:
        copy.start()
    copies[0].start()
    for copy in copies:
        copy.wait()


def sign_body(lay, starts, scale, terms, left_hbm, *refs):
    sources, (out, pool, left, result, sems, out_sems) = refs[: len(starts)], refs[len(starts) :]
    copies = load_pool([*sources], starts, pool, sems)
    own = pltpu.make_async_copy(left_hbm, left, sems.at[len(starts)])
    own.start()
    for copy in copies:
        copy.wait()
    own.wait()

    def finish(o, total):
        value = 1.5 * left[o].astype(jnp.float32)
        if total is not None:
            value = value - total * scale
        used = terms[o * TERMS + TERMS - 1] == 1
        result[o] = jnp.where(used, value, 0.0).astype(result.dtype)

    products(lay, terms, left, pool, finish)
    copy = pltpu.make_async_copy(result, out, out_sems)
    copy.start()
    copy.wait()


def local(x_blocks, columns, filter_ids):
    grp_count = lax.axis_size("grp")
    col_count = lax.axis_size("col")
    rows, rows_c, slots = x_blocks.shape[:3]
    block = x_blocks.shape[3:]
    assert rows_c == 1 and col_count % 2 == 0 and filter_ids.shape[2] == slots and slots <= 6
    lay = Layout(rows, slots, col_count, grp_count)
    scale = 0.5 / (slots * block[0])
    sizes = [(*SECOND[s], lay.most - FIRST[s]) for s in range(2)]

    grid = columns.shape[:2]
    at_a = lax.broadcasted_iota(jnp.int32, (*grid, slots), 0)
    at_c = lax.broadcasted_iota(jnp.int32, (*grid, slots), 1)

    def coded(ids):
        da = (ids // col_count - at_a + 1) % grid[0]
        dc = (ids % col_count - at_c + 1) % grid[1]
        code = jnp.where(ids >= 0, da * 5 + dc, -1)
        mask = jnp.sum(jnp.where(ids >= 0, 1 << jnp.maximum(code, 0), 0), axis=2)
        return code, mask

    col_code, col_mask = coded(columns)
    filt_code, filt_mask = coded(filter_ids)
    zero = jnp.zeros_like(col_mask)
    tab = jnp.concatenate(
        [
            *(jnp.pad(code, ((0, 0), (0, 0), (0, 6 - slots)), constant_values=-1) for code in (col_code, filt_code)),
            jnp.stack([col_mask, filt_mask, zero, zero], axis=2),
        ],
        axis=2,
    ).reshape(-1)
    vec = jnp.stack([col_mask, filt_mask, at_a[:, :, 0] % rows, at_c[:, :, 0]]).reshape(4, -1)
    here = jnp.stack([lax.axis_index("grp"), lax.axis_index("col")]).astype(jnp.int32)

    x = x_blocks.reshape(lay.own, *block)
    ranks = pltpu.SMEM((16,), jnp.int32)
    sends0, edges0, picks = pl.pallas_call(
        functools.partial(first_plan_body, lay, FIRST, sizes),
        out_shape=[ints(lay.most), ints(16), ints(2)],
        in_specs=[SMEM, SMEM, VMEM],
        out_specs=[SMEM] * 3,
        scratch_shapes=[ranks],
    )(here, tab, vec)

    ups = [(n, (n + 1) % grp_count) for n in range(grp_count)]
    downs = [((n + 1) % grp_count, n) for n in range(grp_count)]
    swaps = [(n, n ^ 1) for n in range(col_count)]
    offs = [(n, (n - 1 if n % 2 == 0 else n + 1) % col_count) for n in range(col_count)]
    late = slots - lay.edge
    edge_sizes = [lay.edge, late, lay.edge, late] if late else [lay.edge, lay.edge]

    def edge_picks(list_at, out):
        found = []
        for way in range(2):
            for m in range(slots):
                step = len(edge_sizes) // 2
                place = (out + way * step, m) if m < lay.edge else (out + way * step + 1, m - lay.edge)
                found.append((list_at, way * 8 + m, *place))
        return found

    def exchange(source, edges_out, first_out, sends, first, second):
        step = len(edges_out) // 2
        got_off = lax.ppermute(first_out, "col", offs)
        from_top = [lax.ppermute(edges_out[0], "grp", ups)]
        from_bottom = [lax.ppermute(edges_out[step], "grp", downs)]
        got_side = lax.ppermute(source, "col", swaps)
        if late:
            from_top.append(lax.ppermute(edges_out[1], "grp", ups))
            from_bottom.append(lax.ppermute(edges_out[step + 1], "grp", downs))
        parts = [
            (0, lay.own),
            (lay.top, lay.top + lay.edge),
            (lay.bottom, lay.bottom + lay.edge),
        ]
        (second_out,) = pack(
            block,
            [sends],
            [source, from_top[0], from_bottom[0]],
            parts,
            [second],
            [(0, first + j, 0, j) for j in range(second)],
        )
        got_second = lax.ppermute(second_out, "col", offs)
        side_edges = lax.ppermute(jnp.concatenate(from_top + from_bottom), "col", swaps)
        buffers = [source, *from_top, *from_bottom, got_side, side_edges, got_off, got_second]
        starts = [0]
        for buffer in buffers[:-1]:
            starts.append(starts[-1] + buffer.shape[0])
        return buffers, starts

    def stage0(second, x, sends0, edges0, here, tab):
        first_out, *edges_out = pack(
            block,
            [sends0, edges0],
            [x],
            [(0, lay.own)],
            [FIRST[0], *edge_sizes],
            [(0, j, 0, j) for j in range(FIRST[0])] + edge_picks(1, 1),
        )
        sends1, edges1, terms0, terms1 = pl.pallas_call(
            functools.partial(rest_plan_body, lay, FIRST),
            out_shape=[ints(lay.most), ints(16), ints(lay.own * TERMS), ints(lay.own * TERMS)],
            in_specs=[SMEM, SMEM],
            out_specs=[SMEM] * 4,
            scratch_shapes=[
                ranks,
                pltpu.SMEM((3 * (rows + 2) * 8,), jnp.int32),
                pltpu.SMEM((16,), jnp.int32),
            ],
            cost_estimate=pl.CostEstimate(flops=1 << 20, bytes_accessed=1 << 16, transcendentals=0),
        )(here, tab)
        buffers, starts = exchange(x, edges_out, first_out, sends0, FIRST[0], second)
        picks1 = [(0, j, 0, j) for j in range(FIRST[1])] + edge_picks(1, 1)
        pool_size = starts[-1] + second
        square, first1, *edges_out1 = pl.pallas_call(
            functools.partial(square_body, lay, starts, picks1),
            out_shape=[
                jax.ShapeDtypeStruct((n, *block), jnp.bfloat16)
                for n in (lay.own, FIRST[1], *edge_sizes)
            ],
            in_specs=[SMEM] * 3 + [ANY] * len(buffers),
            out_specs=[ANY] * (2 + len(edge_sizes)),
            scratch_shapes=[
                pltpu.VMEM((pool_size, *block), jnp.bfloat16),
                pltpu.VMEM((lay.own, *block), jnp.bfloat16),
                pltpu.SemaphoreType.DMA((len(buffers),)),
                pltpu.SemaphoreType.DMA((1 + len(picks1),)),
            ],
            cost_estimate=pl.CostEstimate(flops=1 << 31, bytes_accessed=1 << 23, transcendentals=0),
        )(terms0, sends1, edges1, *buffers)
        return square, first1, tuple(edges_out1), sends1, terms1

    def stage1(second, x, square, first_out, edges_out, sends1, terms1):
        buffers, starts = exchange(square, list(edges_out), first_out, sends1, FIRST[1], second)
        pool_size = starts[-1] + second
        return pl.pallas_call(
            functools.partial(sign_body, lay, starts, scale),
            out_shape=jax.ShapeDtypeStruct(x.shape, jnp.bfloat16),
            in_specs=[SMEM, ANY] + [ANY] * len(buffers),
            out_specs=ANY,
            scratch_shapes=[
                pltpu.VMEM((pool_size, *block), jnp.bfloat16),
                pltpu.VMEM((lay.own, *block), jnp.bfloat16),
                pltpu.VMEM((lay.own, *block), jnp.bfloat16),
                pltpu.SemaphoreType.DMA((len(buffers) + 1,)),
                pltpu.SemaphoreType.DMA,
            ],
            cost_estimate=pl.CostEstimate(flops=1 << 31, bytes_accessed=1 << 23, transcendentals=0),
        )(terms1, x, *buffers)

    square, first1, edges_out1, sends1, terms1 = lax.switch(
        picks[0], [functools.partial(stage0, size) for size in sizes[0]], x, sends0, edges0, here, tab
    )
    result = lax.switch(
        picks[1],
        [functools.partial(stage1, size) for size in sizes[1]],
        x, square, first1, edges_out1, sends1, terms1,
    )
    return result.reshape(x_blocks.shape)


def solution(mesh):
    return jax.shard_map(
        local,
        mesh=mesh,
        in_specs=(P("grp", "col", None, None, None), P(), P()),
        out_specs=P("grp", "col", None, None, None),
        check_vma=False,
    )
```

```python
import functools

import jax
import jax.numpy as jnp
from jax import lax
from jax.experimental import pallas as pl
from jax.experimental.pallas import tpu as pltpu
from jax.sharding import PartitionSpec as P


FIRST = (10, 12)
SECOND = ((4, 6, 8), (4, 6, 8))

ANY = pl.BlockSpec(memory_space=pl.ANY)
SMEM = pl.BlockSpec(memory_space=pltpu.SMEM)
VMEM = pl.BlockSpec(memory_space=pltpu.VMEM)

LINE = 16
TERMS = 8


class Layout:
    def __init__(self, rows, slots, cols, groups):
        self.rows, self.slots, self.cols, self.groups = rows, slots, cols, groups
        self.grid_a = rows * groups
        self.own = rows * slots
        self.top = self.own
        self.bottom = self.own + slots
        self.side = self.own + 2 * slots
        self.off = 2 * self.side
        self.edge = 4 if slots > 4 else slots
        self.most = self.own + 2 * self.edge

    def line(self, a, c):
        a = jnp.where(a < 0, a + self.grid_a, jnp.where(a >= self.grid_a, a - self.grid_a, a))
        return (a * self.cols + c) * LINE

    def around(self, c):
        even = (c & 1) == 0
        partner = jnp.where(even, c + 1, c - 1)
        other = jnp.where(even, c - 1, c + 1)
        other = jnp.where(other < 0, self.cols - 1, jnp.where(other >= self.cols, 0, other))
        return partner, other, jnp.where(even, 0, 2)


def edge_order(lay, tab, line, codes_at, off_code, first_da, put):
    fits = []
    for m in range(lay.slots):
        code = tab[line + codes_at + m]
        da = (code >= 5).astype(jnp.int32) + (code >= 10).astype(jnp.int32)
        dc = code - 5 * da
        ok = (code >= 0) & ((da == first_da) | (da == 1)) & ((dc == 1) | (dc == off_code))
        fits.append(ok.astype(jnp.int32))
    front, back = jnp.int32(0), sum(fits)
    for m in range(lay.slots):
        put(m, jnp.where(fits[m] == 1, front, back))
        front, back = front + fits[m], back + 1 - fits[m]


def used_masks(lay, tab, a0, consumer, source_code, target_at):
    masks = [jnp.int32(0)] * (lay.rows + 2)
    for i in range(lay.rows):
        line = lay.line(a0 + i, consumer)
        cols_mask = tab[line + 12]
        target = tab[line + target_at] << 6
        for da in range(3):
            code = da * 5 + source_code
            masks[i + da] = masks[i + da] | jnp.where(((cols_mask >> code) & 1) == 1, target >> code, 0)
    return masks


def used_list(lay, tab, a0, source, masks, codes_at, first, put):
    count = jnp.int32(0)
    for ii in [*range(1, lay.rows + 1), 0, lay.rows + 1]:
        if ii == 0:
            count = jnp.maximum(count, first)
        line = lay.line(a0 + ii - 1, source)
        for m in range(lay.slots):
            code = tab[line + codes_at + m]
            hit = ((masks[ii] >> jnp.maximum(code, 0)) & 1) * (code >= 0).astype(jnp.int32)
            put(hit, count, ii, m)
            count = count + hit


def send_plan(lay, here, tab, stage, first, ranks, sends, edges):
    g, c = here[0], here[1]
    _, other, off_code = lay.around(c)
    codes_at, target_at = (0, 13) if stage == 0 else (6, 12)
    a0 = g * lay.rows
    for which, (a, da) in enumerate(((a0 - 1, 2), (a0 + lay.rows, 0))):

        def put_rank(m, rank, at=which * 8):
            ranks[at + m] = rank

        edge_order(lay, tab, lay.line(a, c), codes_at, off_code, da, put_rank)
    for which, (row, da) in enumerate(((lay.rows - 1, 2), (0, 0))):

        def put_edge(m, rank, at=which * 8, row=row):
            edges[at + rank] = row * lay.slots + m

        edge_order(lay, tab, lay.line(a0 + row, c), codes_at, off_code, da, put_edge)
    for j in range(lay.most):
        sends[j] = 0

    def put(hit, count, ii, m):
        if ii == 0:
            index = lay.top + ranks[m]
        elif ii == lay.rows + 1:
            index = lay.bottom + ranks[8 + m]
        else:
            index = (ii - 1) * lay.slots + m

        @pl.when(hit == 1)
        def _():
            sends[count] = index

    masks = used_masks(lay, tab, a0, other, off_code_of_source(off_code), target_at)
    used_list(lay, tab, a0, c, masks, codes_at, first, put)


def off_code_of_source(off_code):
    return 2 - off_code


def term_plan(lay, here, tab, stage, first, place, slot_of, terms):
    g, c = here[0], here[1]
    partner, other, off_code = lay.around(c)
    codes_at, target_at, goal_at = (0, 13, 6) if stage == 0 else (6, 12, 0)
    a0 = g * lay.rows
    span = lay.rows + 2
    for side, column, own_off in ((0, c, off_code), (1, partner, 2 - off_code)):
        base = side * lay.side
        for ii in range(1, lay.rows + 1):
            for m in range(lay.slots):
                place[(side * span + ii) * 8 + m] = base + (ii - 1) * lay.slots + m
        for ii, da, start in ((0, 2, lay.top), (lay.rows + 1, 0, lay.bottom)):

            def put_rank(m, rank, at=(side * span + ii) * 8, start=base + start):
                place[at + m] = start + rank

            edge_order(lay, tab, lay.line(a0 + ii - 1, column), codes_at, own_off, da, put_rank)

    def put(hit, count, ii, m):
        place[(2 * span + ii) * 8 + m] = lay.off + count

    masks = used_masks(lay, tab, a0, c, off_code, target_at)
    used_list(lay, tab, a0, other, masks, codes_at, first, put)

    for i in range(lay.rows):
        line = lay.line(a0 + i, c)
        target = tab[line + target_at] << 6
        for f in range(lay.slots):
            code = tab[line + goal_at + f]
            at = (i * lay.slots + f) * TERMS
            terms[at] = 0
            terms[at + TERMS - 1] = (code >= 0).astype(jnp.int32)

            @pl.when(code >= 0)
            def _(code=code, f=f):
                slot_of[code] = f

        def one_slot(k, carry, i=i, line=line, target=target):
            code = tab[line + k]

            @pl.when(code >= 0)
            def _():
                da = (code >= 5).astype(jnp.int32) + (code >= 10).astype(jnp.int32)
                dc = code - 5 * da
                side = jnp.where(dc == 1, 0, jnp.where(dc == off_code, 2, 1))
                column = jnp.where(side == 0, c, jnp.where(side == 1, partner, other))
                source = lay.line(a0 + i + da - 1, column)
                place_at = (side * span + i + da) * 8
                wanted = target >> code
                for m in range(lay.slots):
                    there = tab[source + codes_at + m]
                    hit = ((wanted >> jnp.maximum(there, 0)) & 1) * (there >= 0).astype(jnp.int32)

                    @pl.when(hit == 1)
                    def _(there=there, m=m):
                        at = (i * lay.slots + slot_of[code + there - 6]) * TERMS
                        count = terms[at] + 1
                        terms[at] = count
                        terms[at + count] = (i * lay.slots + k) * 256 + place[place_at + m]

            return carry

        lax.fori_loop(0, lay.slots, one_slot, 0)


def needed_second(lay, vec, stage, first):
    shape = (8, vec.shape[1])
    cols_mask, filt_mask, i, c = (jnp.broadcast_to(vec[n : n + 1, :], shape) for n in range(4))
    stored, goal = (cols_mask, filt_mask) if stage == 0 else (filt_mask, cols_mask)
    total = shape[1]
    width = lay.cols

    def count(bits):
        return sum((bits >> (da * 5 + dc)) & 1 for da in range(3) for dc in range(3))

    def moved(value, by):
        return value if by % total == 0 else pltpu.roll(value, by % total, 1)

    most = jnp.zeros(shape, jnp.int32)
    for source_code in (0, 2):
        bits = []
        for da in range(3):
            code = da * 5 + source_code
            value = jnp.where(((cols_mask >> code) & 1) == 1, (goal << 6) >> code, 0)
            by = (da - 1) * width + source_code - 1
            wraps = c == (0 if source_code == 2 else width - 1)
            back = by - width if source_code == 2 else by + width
            bits.append(jnp.where(wraps, moved(value, back), moved(value, by)) & stored)
        beside = bits[1] | jnp.where(i < lay.rows - 1, bits[0], 0) | jnp.where(i > 0, bits[2], 0)
        beside = count(beside)
        top = count(jnp.where(i == lay.rows - 1, bits[0], 0))
        bottom = count(jnp.where(i == 0, bits[2], 0))
        sides = sum(moved(beside, -j * width) for j in range(lay.rows))
        corners = moved(top, width) + moved(bottom, -lay.rows * width)
        need = jnp.maximum(sides, first) + corners - first
        counts = (i == 0) & ((c & 1) == (0 if source_code == 2 else 1))
        most = jnp.maximum(most, jnp.where(counts, need, 0))
    return jnp.max(most)


def first_plan_body(lay, firsts, sizes, here, tab, vec, sends, edges, picks, ranks):
    send_plan(lay, here, tab, 0, firsts[0], ranks, sends, edges)
    for stage in range(2):
        need = needed_second(lay, vec[...], stage, firsts[stage])
        picks[stage] = sum((need > size).astype(jnp.int32) for size in sizes[stage][:-1])


def rest_plan_body(lay, firsts, here, tab, sends, edges, terms0, terms1, ranks, place, slot_of):
    send_plan(lay, here, tab, 1, firsts[1], ranks, sends, edges)
    term_plan(lay, here, tab, 0, firsts[0], place, slot_of, terms0)
    term_plan(lay, here, tab, 1, firsts[1], place, slot_of, terms1)


def ints(*shape):
    return jax.ShapeDtypeStruct(shape, jnp.int32)


def pack_body(parts, picks, sends, *refs):
    sources, rest = refs[: len(parts)], refs[len(parts) :]
    outs, (held, sems_in, sems_out) = rest[:-3], rest[-3:]
    for j, (list_ref, at, _, _) in enumerate(picks):
        index = sends[list_ref][at]
        for source, (low, high) in zip(sources, parts):

            @pl.when((index >= low) & (index < high))
            def _(source=source, low=low, j=j, index=index):
                pltpu.make_async_copy(source.at[index - low], held.at[j], sems_in.at[j]).start()

    for j, (_, _, out, at_out) in enumerate(picks):
        pltpu.make_async_copy(sources[0].at[0], held.at[j], sems_in.at[j]).wait()
        pltpu.make_async_copy(held.at[j], outs[out].at[at_out], sems_out.at[j]).start()
    for j, (_, _, out, at_out) in enumerate(picks):
        pltpu.make_async_copy(held.at[j], outs[out].at[at_out], sems_out.at[j]).wait()


def pack(block, lists, sources, parts, sizes, picks):
    def body(*refs):
        pack_body(parts, picks, refs[: len(lists)], *refs[len(lists) :])

    return pl.pallas_call(
        body,
        out_shape=[jax.ShapeDtypeStruct((size, *block), jnp.bfloat16) for size in sizes],
        in_specs=[SMEM] * len(lists) + [ANY] * len(sources),
        out_specs=[ANY] * len(sizes),
        scratch_shapes=[
            pltpu.VMEM((len(picks), *block), jnp.bfloat16),
            pltpu.SemaphoreType.DMA((len(picks),)),
            pltpu.SemaphoreType.DMA((len(picks),)),
        ],
        cost_estimate=pl.CostEstimate(
            flops=1 << 20, bytes_accessed=4 * len(picks) * block[0] * block[1], transcendentals=0
        ),
    )(*lists, *sources)


def products(lay, terms, left, pool, finish):
    def one(o, carry):
        at = o * TERMS
        count = terms[at]
        for n in range(lay.slots + 1):

            @pl.when(count == n)
            def _(n=n):
                if n == 0:
                    finish(o, None)
                    return
                lefts, rights = [], []
                for e in range(n):
                    term = terms[at + 1 + e]
                    lefts.append(left[term >> 8])
                    rights.append(pool[term & 255])
                joined = lefts[0] if n == 1 else jnp.concatenate(lefts, axis=1)
                stacked = rights[0] if n == 1 else jnp.concatenate(rights, axis=0)
                finish(o, jnp.dot(joined, stacked, preferred_element_type=jnp.float32))

        return carry

    lax.fori_loop(0, lay.own, one, 0)


def load_pool(sources, starts, pool, sems):
    copies = [
        pltpu.make_async_copy(source, pool.at[pl.ds(start, source.shape[0])], sems.at[n])
        for n, (source, start) in enumerate(zip(sources, starts))
    ]
    for copy in copies:
        copy.start()
    return copies


def square_body(lay, starts, picks, terms, sends, edges, *refs):
    sources, rest = refs[: len(starts)], refs[len(starts) :]
    outs, (pool, square, sems, out_sems) = rest[:-4], rest[-4:]
    for copy in load_pool(sources, starts, pool, sems):
        copy.wait()

    def finish(o, total):
        if total is None:
            square[o] = jnp.zeros(square.shape[1:], square.dtype)
        else:
            square[o] = total.astype(square.dtype)

    products(lay, terms, pool, pool, finish)
    lists = (sends, edges)
    copies = [pltpu.make_async_copy(square, outs[0], out_sems.at[0])]
    for j, (list_at, at, out, at_out) in enumerate(picks):
        copies.append(
            pltpu.make_async_copy(
                square.at[lists[list_at][at]], outs[out + 1].at[at_out], out_sems.at[j + 1]
            )
        )
    for copy in copies[1:]:
        copy.start()
    copies[0].start()
    for copy in copies:
        copy.wait()


def sign_body(lay, starts, scale, terms, left_hbm, *refs):
    sources, (out, pool, left, result, sems, out_sems) = refs[: len(starts)], refs[len(starts) :]
    copies = load_pool([*sources], starts, pool, sems)
    own = pltpu.make_async_copy(left_hbm, left, sems.at[len(starts)])
    own.start()
    for copy in copies:
        copy.wait()
    own.wait()

    def finish(o, total):
        value = 1.5 * left[o].astype(jnp.float32)
        if total is not None:
            value = value - total * scale
        used = terms[o * TERMS + TERMS - 1] == 1
        result[o] = jnp.where(used, value, 0.0).astype(result.dtype)

    products(lay, terms, left, pool, finish)
    copy = pltpu.make_async_copy(result, out, out_sems)
    copy.start()
    copy.wait()


def local(x_blocks, columns, filter_ids):
    grp_count = lax.axis_size("grp")
    col_count = lax.axis_size("col")
    rows, rows_c, slots = x_blocks.shape[:3]
    block = x_blocks.shape[3:]
    assert rows_c == 1 and col_count % 2 == 0 and filter_ids.shape[2] == slots and slots <= 6
    lay = Layout(rows, slots, col_count, grp_count)
    scale = 0.5 / (slots * block[0])
    sizes = [(*SECOND[s], lay.most - FIRST[s]) for s in range(2)]

    grid = columns.shape[:2]
    at_a = lax.broadcasted_iota(jnp.int32, (*grid, slots), 0)
    at_c = lax.broadcasted_iota(jnp.int32, (*grid, slots), 1)

    def coded(ids):
        da = (ids // col_count - at_a + 1) % grid[0]
        dc = (ids % col_count - at_c + 1) % grid[1]
        code = jnp.where(ids >= 0, da * 5 + dc, -1)
        mask = jnp.sum(jnp.where(ids >= 0, 1 << jnp.maximum(code, 0), 0), axis=2)
        return code, mask

    col_code, col_mask = coded(columns)
    filt_code, filt_mask = coded(filter_ids)
    zero = jnp.zeros_like(col_mask)
    tab = jnp.concatenate(
        [
            *(jnp.pad(code, ((0, 0), (0, 0), (0, 6 - slots)), constant_values=-1) for code in (col_code, filt_code)),
            jnp.stack([col_mask, filt_mask, zero, zero], axis=2),
        ],
        axis=2,
    ).reshape(-1)
    vec = jnp.stack([col_mask, filt_mask, at_a[:, :, 0] % rows, at_c[:, :, 0]]).reshape(4, -1)
    here = jnp.stack([lax.axis_index("grp"), lax.axis_index("col")]).astype(jnp.int32)

    x = x_blocks.reshape(lay.own, *block)
    ranks = pltpu.SMEM((16,), jnp.int32)
    sends0, edges0, picks = pl.pallas_call(
        functools.partial(first_plan_body, lay, FIRST, sizes),
        out_shape=[ints(lay.most), ints(16), ints(2)],
        in_specs=[SMEM, SMEM, VMEM],
        out_specs=[SMEM] * 3,
        scratch_shapes=[ranks],
    )(here, tab, vec)

    ups = [(n, (n + 1) % grp_count) for n in range(grp_count)]
    downs = [((n + 1) % grp_count, n) for n in range(grp_count)]
    swaps = [(n, n ^ 1) for n in range(col_count)]
    offs = [(n, (n - 1 if n % 2 == 0 else n + 1) % col_count) for n in range(col_count)]
    late = slots - lay.edge
    edge_sizes = [lay.edge, late, lay.edge, late] if late else [lay.edge, lay.edge]

    def edge_picks(list_at, out):
        found = []
        for way in range(2):
            for m in range(slots):
                step = len(edge_sizes) // 2
                place = (out + way * step, m) if m < lay.edge else (out + way * step + 1, m - lay.edge)
                found.append((list_at, way * 8 + m, *place))
        return found

    def exchange(source, edges_out, first_out, sends, first, second, ready):
        step = len(edges_out) // 2
        got_off = lax.ppermute(first_out, "col", offs)
        from_top = [lax.ppermute(edges_out[0], "grp", ups)]
        from_bottom = [lax.ppermute(edges_out[step], "grp", downs)]
        got_side = lax.ppermute(source, "col", swaps)
        if late:
            from_top.append(lax.ppermute(edges_out[1], "grp", ups))
            from_bottom.append(lax.ppermute(edges_out[step + 1], "grp", downs))
        parts = [
            (0, lay.own),
            (lay.top, lay.top + lay.edge),
            (lay.bottom, lay.bottom + lay.edge),
        ]
        sends, ready = lax.optimization_barrier((sends, ready))
        (second_out,) = pack(
            block,
            [sends],
            [source, from_top[0], from_bottom[0]],
            parts,
            [second],
            [(0, first + j, 0, j) for j in range(second)],
        )
        got_second = lax.ppermute(second_out, "col", offs)
        tails = from_top[1:] + from_bottom[1:]
        if tails:
            second_out, *tails = lax.optimization_barrier((second_out, *tails))
            half = len(tails) // 2
            from_top[1:], from_bottom[1:] = tails[:half], tails[half:]
        joined = jnp.concatenate(from_top + from_bottom)
        side_edges = lax.ppermute(joined, "col", swaps)
        buffers = [source, *from_top, *from_bottom, got_side, side_edges, got_off, got_second]
        starts = [0]
        for buffer in buffers[:-1]:
            starts.append(starts[-1] + buffer.shape[0])
        return buffers, starts, ready

    def stage0(second, x, sends0, edges0, here, tab):
        first_out, *edges_out = pack(
            block,
            [sends0, edges0],
            [x],
            [(0, lay.own)],
            [FIRST[0], *edge_sizes],
            [(0, j, 0, j) for j in range(FIRST[0])] + edge_picks(1, 1),
        )
        plan = pl.pallas_call(
            functools.partial(rest_plan_body, lay, FIRST),
            name="rest_plan",
            out_shape=[ints(lay.most), ints(16), ints(lay.own * TERMS), ints(lay.own * TERMS)],
            in_specs=[SMEM, SMEM],
            out_specs=[SMEM] * 4,
            scratch_shapes=[
                ranks,
                pltpu.SMEM((3 * (rows + 2) * 8,), jnp.int32),
                pltpu.SMEM((16,), jnp.int32),
            ],
            cost_estimate=pl.CostEstimate(flops=1 << 20, bytes_accessed=1 << 16, transcendentals=0),
        )
        ready = plan(here, tab)
        buffers, starts, ready = exchange(x, edges_out, first_out, sends0, FIRST[0], second, ready)
        sends1, edges1, terms0, terms1 = ready
        picks1 = [(0, j, 0, j) for j in range(FIRST[1])] + edge_picks(1, 1)
        pool_size = starts[-1] + second
        square, first1, *edges_out1 = pl.pallas_call(
            functools.partial(square_body, lay, starts, picks1),
            out_shape=[
                jax.ShapeDtypeStruct((n, *block), jnp.bfloat16)
                for n in (lay.own, FIRST[1], *edge_sizes)
            ],
            in_specs=[SMEM] * 3 + [ANY] * len(buffers),
            out_specs=[ANY] * (2 + len(edge_sizes)),
            scratch_shapes=[
                pltpu.VMEM((pool_size, *block), jnp.bfloat16),
                pltpu.VMEM((lay.own, *block), jnp.bfloat16),
                pltpu.SemaphoreType.DMA((len(buffers),)),
                pltpu.SemaphoreType.DMA((1 + len(picks1),)),
            ],
            cost_estimate=pl.CostEstimate(flops=1 << 31, bytes_accessed=1 << 23, transcendentals=0),
        )(terms0, sends1, edges1, *buffers)
        return square, first1, tuple(edges_out1), sends1, terms1

    def stage1(second, x, square, first_out, edges_out, sends1, terms1):
        buffers, starts, _ = exchange(square, list(edges_out), first_out, sends1, FIRST[1], second, ())
        pool_size = starts[-1] + second
        return pl.pallas_call(
            functools.partial(sign_body, lay, starts, scale),
            out_shape=jax.ShapeDtypeStruct(x.shape, jnp.bfloat16),
            in_specs=[SMEM, ANY] + [ANY] * len(buffers),
            out_specs=ANY,
            scratch_shapes=[
                pltpu.VMEM((pool_size, *block), jnp.bfloat16),
                pltpu.VMEM((lay.own, *block), jnp.bfloat16),
                pltpu.VMEM((lay.own, *block), jnp.bfloat16),
                pltpu.SemaphoreType.DMA((len(buffers) + 1,)),
                pltpu.SemaphoreType.DMA,
            ],
            cost_estimate=pl.CostEstimate(flops=1 << 31, bytes_accessed=1 << 23, transcendentals=0),
        )(terms1, x, *buffers)

    def layered(stage, size):
        def run(*args):
            return (stage0, stage1)[stage](size, *args)

        return run

    square, first1, edges_out1, sends1, terms1 = lax.switch(
        picks[0], [layered(0, size) for size in sizes[0]], x, sends0, edges0, here, tab
    )
    result = lax.switch(
        picks[1],
        [layered(1, size) for size in sizes[1]],
        x, square, first1, edges_out1, sends1, terms1,
    )
    return result.reshape(x_blocks.shape)


def solution(mesh):
    return jax.shard_map(
        local,
        mesh=mesh,
        in_specs=(P("grp", "col", None, None, None), P(), P()),
        out_specs=P("grp", "col", None, None, None),
        check_vma=False,
    )
```
